32 devices in a mesh: dp: 16 (over z, y, x), seq: 2 (over core).
Axes of the slice: x: 2, y: 2, z: 4, core: 2. Of those that a mesh axis runs over, the one named last changes fastest.
Arguments:
- activations: bfloat16 [4096, 8192], P(('dp', 'seq')), may hold values from -6 to 6
- queries: bfloat16 [4096, 8192], P(('dp', 'seq')), may hold values from -180 to 180
- keys: bfloat16 [4096, 1024], P(('dp', 'seq')), may hold values from -6 to 6
- out_grad: bfloat16 [4096, 8192], P(('dp', 'seq')), may hold values from -0.078125 to 0.078125
- layout: int32 [8192], replicated, may hold values from 0 to 8191, each once
Outputs:
- value_weight_grad: float32 [8192, 1024], P(('dp', 'seq'))
The draws below stay inside these ranges and needn't reach their ends.
Inputs may be any that keep to these rules, and one draw needn't show every extreme that they name: `layout`: every row number 0 to 8191 appears exactly once.
All inputs are finite; a program needn't handle non-finite values.
Results may differ from the reference program's by a relative error of at most 0.0049.
Values may be sent and summed in bfloat16 or wider, within the bound.
A program may use at most 128 MiB of HBM per device.

```python
import jax
import jax.numpy as jnp
from jax import lax

D = 8192
H = 64
KVH = 8
HD = 128
LENGTH = 256
TOKENS = 4096


def draw_pair(key):
    base_keys = jnp.clip(jax.random.normal(jax.random.fold_in(key, 11), (TOKENS, KVH * HD), jnp.float32), -6.0, 6.0)
    fresh = jnp.clip(jax.random.normal(jax.random.fold_in(key, 12), (TOKENS, H * HD), jnp.float32), -6.0, 6.0)
    return (fresh, base_keys)


def draw_queries(key, part):
    return draw_pair(key)[0].astype(jnp.bfloat16)


def draw_keys(key, part):
    return draw_pair(key)[1].astype(jnp.bfloat16)


def raised(result, own_key, source, target, blocks, factor):
    owner, partner = [(jnp.arange(result.shape[position]) // (result.shape[position] // blocks)).reshape([-1 if axis == position else 1 for axis in range(result.ndim)]) for position in (source, target)]
    chosen = jax.random.permutation(own_key, blocks)[partner]
    strong = (owner == chosen) | (owner == (partner + blocks // 2) % blocks)
    return jnp.where(strong, factor * result, result)


def block_scale(own_key, dims, split, smallest, high):
    gain, own = 1.0, jax.random.fold_in(own_key, 6)
    for dim, parts in split:
        draws = jnp.exp(jax.random.uniform(jax.random.fold_in(own, dim), (parts,), jnp.float32, smallest / len(split), high / len(split)))
        gain = gain * jnp.repeat(draws, dims[dim] // parts).reshape([-1 if axis == dim else 1 for axis in range(len(dims))])
    return gain


def bell_draw(own_key, extent, spread, limit, shards=(), kind=jnp.bfloat16):
    drawn = spread * jax.random.normal(own_key, extent, jnp.float32)
    if shards:
        drawn = drawn * block_scale(own_key, extent, shards, -0.22, 0.18)
    return jnp.clip(drawn, -limit, limit).astype(kind)


def gaussian_with(rng, extent, width, reach, cuts, heavy, held_as=jnp.bfloat16):
    array = width * jax.random.normal(rng, extent, jnp.float32)
    if cuts:
        array = array * block_scale(rng, extent, cuts, -0.22, 0.18)
    return jnp.clip(raised(array, jax.random.fold_in(rng, 3), *heavy), -reach, reach).astype(held_as)


def setup_inputs(seed: int = 0) -> dict:
    streams_of = jax.random.split(jax.random.key(seed), 6)
    activations = gaussian_with(streams_of[0], (TOKENS, D), 1.0, 6.0, ((0, 32),), (0, 1, 32, 2.75))
    queries = draw_queries(jax.random.fold_in(streams_of[5], 71), 0)
    keys = draw_keys(jax.random.fold_in(streams_of[5], 71), 0)
    out_grad = bell_draw(streams_of[3], (TOKENS, H * HD), ((8 * TOKENS) ** -0.5), 0.078125, ((0, 32),))
    layout = jax.random.permutation(streams_of[4], D).astype(jnp.int32)
    return {"activations": activations, "queries": queries, "keys": keys, "out_grad": out_grad, "layout": layout}


def value_grads(seq_queries, seq_keys, seq_grads):
    length = seq_queries.shape[0]
    per_group = H // KVH
    inv_root = 1.0 / float(HD) ** 0.5
    places = jnp.arange(length)
    allowed = places[:, None] >= places[None, :]
    pieces = []
    for group_index in range(KVH):
        offset = group_index * per_group * HD
        query_block = seq_queries[:, offset:offset + per_group * HD].reshape(length, per_group, HD).astype(jnp.float32)
        grad_block = seq_grads[:, offset:offset + per_group * HD].reshape(length, per_group, HD).astype(jnp.float32)
        key_block = seq_keys[:, group_index * HD:(group_index + 1) * HD].astype(jnp.float32)
        scores = jnp.einsum("igd,jd->gij", query_block, key_block) * inv_root
        scores = jnp.where(allowed[None], scores, -jnp.inf)
        weights = lax.optimization_barrier(jax.nn.softmax(scores, axis=-1).astype(jnp.bfloat16))
        pieces.append(jnp.einsum("gij,igd->jd", weights.astype(jnp.float32), grad_block))
    return jnp.concatenate(pieces, axis=1)


def reference(activations, queries, keys, out_grad, layout):
    count_seqs = activations.shape[0] // LENGTH

    def add_sequence(seq_number, grand_sum):
        first_row = (seq_number * LENGTH).astype(jnp.int32)
        seq_rows = lax.dynamic_slice_in_dim(activations, first_row, LENGTH, 0)
        seq_queries = lax.dynamic_slice_in_dim(queries, first_row, LENGTH, 0)
        seq_keys = lax.dynamic_slice_in_dim(keys, first_row, LENGTH, 0)
        seq_grads = lax.dynamic_slice_in_dim(out_grad, first_row, LENGTH, 0)
        value_grad = value_grads(seq_queries, seq_keys, seq_grads).astype(jnp.bfloat16)
        columns = jnp.take(seq_rows, layout.astype(jnp.int32), axis=1)
        row_term = jnp.dot(columns.T, value_grad, preferred_element_type=jnp.float32)
        row_term = lax.optimization_barrier(row_term.astype(jnp.bfloat16))
        return grand_sum + row_term.astype(jnp.float32)

    return lax.fori_loop(0, count_seqs, add_sequence, jnp.zeros((D, KVH * HD), jnp.float32))
```

```python
import functools

import jax
import jax.numpy as jnp
from jax import lax
from jax.experimental import pallas as pl
from jax.experimental.pallas import tpu as pltpu
from jax.sharding import PartitionSpec as P

H = 64
KVH = 8
HD = 128
AXES = ("dp", "seq")


def passed_along(value, axis, steps):
    count = lax.axis_size(axis)
    initial, last = (max(0, -steps), min(count, count - steps))
    return lax.ppermute(value, axis, [(source, source + steps) for source in range(initial, last)])


def gather_kernel(layout_ref, act_ref, out_ref, flipped, picked):
    width = act_ref.shape[1]
    step = 512

    def flip(i, carry):
        at = pl.multiple_of(i * step, step)
        flipped[pl.ds(at, step), :] = act_ref[:, pl.ds(at, step)].astype(jnp.float32).T
        return carry

    lax.fori_loop(0, width // step, flip, 0)
    rows = 256

    def pick(i, carry):
        at = pl.multiple_of(i * rows, rows)

        def some(j, inner):
            first = pl.multiple_of(j * 32, 32)
            for k in range(32):
                picked[pl.ds(first + k, 1), :] = flipped[pl.ds(layout_ref[at + first + k], 1), :]
            return inner

        lax.fori_loop(0, rows // 32, some, 0)
        out_ref[pl.ds(at, rows), :] = picked[...].astype(jnp.bfloat16)
        return carry

    lax.fori_loop(0, width // rows, pick, 0)


def gathered(activations, layout):
    tokens, width = activations.shape
    return pl.pallas_call(
        gather_kernel,
        out_shape=jax.ShapeDtypeStruct((width, tokens), jnp.bfloat16),
        in_specs=[
            pl.BlockSpec(memory_space=pltpu.SMEM),
            pl.BlockSpec(memory_space=pltpu.VMEM),
        ],
        out_specs=pl.BlockSpec(memory_space=pltpu.VMEM),
        scratch_shapes=[
            pltpu.VMEM((width, tokens), jnp.float32),
            pltpu.VMEM((256, tokens), jnp.float32),
        ],
        cost_estimate=pl.CostEstimate(flops=10**7, bytes_accessed=2 * 2**20, transcendentals=0),
    )(layout, activations)


def attention_kernel(q_ref, early_ref, keys_ref, grad_ref, out_ref, *, per_group):
    tokens = q_ref.shape[0]
    seq_index = lax.axis_index("seq")
    both_keys = jnp.concatenate([early_ref[...], keys_ref[...]], axis=0)
    place = lax.broadcasted_iota(jnp.int32, (tokens, 2 * tokens), 0)
    other = lax.broadcasted_iota(jnp.int32, (tokens, 2 * tokens), 1)
    allowed = (other <= place + tokens) & (other >= jnp.where(seq_index == 0, tokens, 0))
    total = jnp.zeros((2 * tokens, HD), jnp.float32)
    for head in range(per_group):
        columns = slice(head * HD, (head + 1) * HD)
        scores = lax.dot_general(
            q_ref[:, columns], both_keys, (((1,), (1,)), ((), ())),
            preferred_element_type=jnp.float32,
        ) * (1.0 / float(HD) ** 0.5)
        scores = jnp.where(allowed, scores, -jnp.inf)
        powers = jnp.exp(scores - jnp.max(scores, axis=1, keepdims=True))
        weights = (powers / jnp.sum(powers, axis=1, keepdims=True)).astype(jnp.bfloat16)
        total += lax.dot_general(
            weights, grad_ref[:, columns], (((0,), (0,)), ((), ())),
            preferred_element_type=jnp.float32,
        )
    out_ref[...] = total


def partial_values(queries, earlier, keys, out_grad):
    tokens = queries.shape[0]
    per_group = H // KVH
    wide = pl.BlockSpec((tokens, per_group * HD), lambda g: (0, g))
    narrow = pl.BlockSpec((tokens, HD), lambda g: (0, g))
    return pl.pallas_call(
        functools.partial(attention_kernel, per_group=per_group),
        grid=(KVH,),
        out_shape=jax.ShapeDtypeStruct((2 * tokens, KVH * HD), jnp.float32),
        in_specs=[wide, narrow, narrow, wide],
        out_specs=pl.BlockSpec((2 * tokens, HD), lambda g: (0, g)),
        cost_estimate=pl.CostEstimate(
            flops=8 * H * HD * tokens * tokens, bytes_accessed=6 * 2**20, transcendentals=2**21
        ),
    )(queries, earlier, keys, out_grad)


def body(activations, queries, keys, out_grad, layout):
    rows_here = activations.shape[0]
    devices = lax.axis_size("dp") * lax.axis_size("seq")
    columns = gathered(activations, layout)
    owned = lax.all_to_all(columns, AXES, 0, 0, tiled=True)
    earlier = passed_along(keys, "seq", 1)
    partial = partial_values(queries, earlier, keys, out_grad)
    returned = passed_along(partial[:rows_here], "seq", -1)
    value_grad = (partial[rows_here:] + returned).astype(jnp.bfloat16)
    values = lax.all_gather(value_grad, AXES, axis=0, tiled=True)
    owned = owned.reshape(devices, -1, rows_here)
    return jnp.einsum(
        "srt,stc->rc",
        owned,
        values.reshape(devices, rows_here, -1),
        preferred_element_type=jnp.float32,
    )


def solution(mesh):
    return jax.shard_map(
        body,
        mesh=mesh,
        in_specs=(P(AXES, None),) * 4 + (P(),),
        out_specs=P(AXES, None),
        check_vma=False,
    )
```

```python
import functools

import jax
import jax.numpy as jnp
from jax import lax
from jax.experimental import pallas as pl
from jax.experimental.pallas import tpu as pltpu
from jax.sharding import PartitionSpec as P

H = 64
KVH = 8
HD = 128


def passed_along(value, axis, steps):
    count = lax.axis_size(axis)
    initial, last = (max(0, -steps), min(count, count - steps))
    return lax.ppermute(value, axis, [(source, source + steps) for source in range(initial, last)])


def gather_kernel(layout_ref, act_ref, far_ref, near_ref, flipped, picked):
    width = act_ref.shape[1]
    step = 512

    def flip(i, carry):
        at = pl.multiple_of(i * step, step)
        flipped[pl.ds(at, step), :] = act_ref[:, pl.ds(at, step)].astype(jnp.float32).T
        return carry

    lax.fori_loop(0, width // step, flip, 0)
    rows = 256
    for part, out_ref in enumerate((far_ref, near_ref)):
        base = part * (width // 2)

        def pick(i, carry):
            at = pl.multiple_of(i * rows, rows)

            def some(j, inner):
                first = pl.multiple_of(j * 32, 32)
                for k in range(32):
                    row = layout_ref[base + at + first + k]
                    picked[pl.ds(first + k, 1), :] = flipped[pl.ds(row, 1), :]
                return inner

            lax.fori_loop(0, rows // 32, some, 0)
            out_ref[pl.ds(at, rows), :] = picked[...].astype(jnp.bfloat16)
            return carry

        lax.fori_loop(0, width // 2 // rows, pick, 0)


def gathered(activations, layout):
    tokens, width = activations.shape
    return pl.pallas_call(
        gather_kernel,
        out_shape=[jax.ShapeDtypeStruct((width // 2, tokens), jnp.bfloat16)] * 2,
        in_specs=[
            pl.BlockSpec(memory_space=pltpu.SMEM),
            pl.BlockSpec(memory_space=pltpu.VMEM),
        ],
        out_specs=[pl.BlockSpec(memory_space=pltpu.VMEM)] * 2,
        scratch_shapes=[
            pltpu.VMEM((width, tokens), jnp.float32),
            pltpu.VMEM((256, tokens), jnp.float32),
        ],
        cost_estimate=pl.CostEstimate(flops=10**10, bytes_accessed=30 * 2**20, transcendentals=0),
    )(layout, activations)


def attention_kernel(q_ref, early_ref, keys_ref, grad_ref, out_ref, *, per_group):
    tokens = q_ref.shape[0]
    seq_index = lax.axis_index("seq")
    both_keys = jnp.concatenate([early_ref[...], keys_ref[...]], axis=0)
    place = lax.broadcasted_iota(jnp.int32, (tokens, 2 * tokens), 0)
    other = lax.broadcasted_iota(jnp.int32, (tokens, 2 * tokens), 1)
    allowed = (other <= place + tokens) & (other >= jnp.where(seq_index == 0, tokens, 0))
    total = jnp.zeros((2 * tokens, HD), jnp.float32)
    for head in range(per_group):
        columns = slice(head * HD, (head + 1) * HD)
        scores = lax.dot_general(
            q_ref[:, columns], both_keys, (((1,), (1,)), ((), ())),
            preferred_element_type=jnp.float32,
        ) * (1.0 / float(HD) ** 0.5)
        scores = jnp.where(allowed, scores, -jnp.inf)
        powers = jnp.exp(scores - jnp.max(scores, axis=1, keepdims=True))
        weights = (powers / jnp.sum(powers, axis=1, keepdims=True)).astype(jnp.bfloat16)
        total += lax.dot_general(
            weights, grad_ref[:, columns], (((0,), (0,)), ((), ())),
            preferred_element_type=jnp.float32,
        )
    out_ref[...] = total


def partial_values(queries, earlier, keys, out_grad):
    tokens = queries.shape[0]
    per_group = H // KVH
    wide = pl.BlockSpec((tokens, per_group * HD), lambda g: (0, g))
    narrow = pl.BlockSpec((tokens, HD), lambda g: (0, g))
    return pl.pallas_call(
        functools.partial(attention_kernel, per_group=per_group),
        grid=(KVH,),
        out_shape=jax.ShapeDtypeStruct((2 * tokens, KVH * HD), jnp.float32),
        in_specs=[wide, narrow, narrow, wide],
        out_specs=pl.BlockSpec((2 * tokens, HD), lambda g: (0, g)),
        cost_estimate=pl.CostEstimate(
            flops=8 * H * HD * tokens * tokens, bytes_accessed=6 * 2**20, transcendentals=2**21
        ),
    )(queries, earlier, keys, out_grad)


def sum_kernel(*refs, orders, add):
    owned_ref = refs[0]
    colors = len(orders)
    mine, theirs = refs[1 : 1 + colors], refs[1 + colors : 1 + 2 * colors]
    out_ref = refs[-1]
    me, seq_index = lax.axis_index("dp"), lax.axis_index("seq")
    for color, order in enumerate(orders):
        width = mine[color].shape[2]
        columns = slice(color * width, (color + 1) * width)
        if add:
            total = refs[-2][:, columns].astype(jnp.float32)
        else:
            total = jnp.zeros((owned_ref.shape[2], width), jnp.float32)
        for place, step in enumerate(order):
            source = me ^ step
            left = jnp.concatenate(
                [owned_ref[source, seq_index], owned_ref[source, 1 - seq_index]], axis=1
            )
            right = jnp.concatenate([mine[color][place], theirs[color][place]], axis=0)
            total += jnp.dot(left, right, preferred_element_type=jnp.float32)
        out_ref[:, columns] = total.astype(out_ref.dtype)


def owner_sum(owned, mine, theirs, orders, arrived, kind):
    rows = owned.shape[2]
    width = sum(piece.shape[2] for piece in mine)
    extra = [] if arrived is None else [arrived]
    operands = [owned, *mine, *theirs, *extra]
    return pl.pallas_call(
        functools.partial(sum_kernel, orders=orders, add=arrived is not None),
        out_shape=jax.ShapeDtypeStruct((rows, width), kind),
        in_specs=[pl.BlockSpec(memory_space=pltpu.VMEM)] * len(operands),
        out_specs=pl.BlockSpec(memory_space=pltpu.VMEM),
        cost_estimate=pl.CostEstimate(
            flops=2 * owned.size * width, bytes_accessed=6 * 2**20, transcendentals=0
        ),
        compiler_params=pltpu.CompilerParams(vmem_limit_bytes=56 * 2**20),
    )(*operands)


def doubled(piece, bits):
    count = lax.axis_size("dp")
    held, order = piece[None], [0]
    for bit in bits:
        arrived = lax.ppermute(held, "dp", [(i, i ^ bit) for i in range(count)])
        held = jnp.concatenate([held, arrived], axis=0)
        order = order + [step ^ bit for step in order]
    return held, tuple(order)


def body(activations, queries, keys, out_grad, layout):
    rows_here = activations.shape[0]
    members, halves = lax.axis_size("dp"), lax.axis_size("half")
    half = lax.axis_index("half")
    split = layout.shape[0] // halves
    turned = jnp.where(half == 0, jnp.roll(layout, -split), layout)
    earlier = passed_along(keys, "seq", 1)
    partial = partial_values(queries, earlier, keys, out_grad)
    returned = passed_along(partial[:rows_here], "seq", -1)
    value_grad = (partial[rows_here:] + returned).astype(jnp.bfloat16)
    bits = [1 << k for k in reversed(range(members.bit_length() - 1))]
    ways = [bits, bits[:-2] + bits[-2:][::-1]]
    width = value_grad.shape[1] // len(ways)
    mine, orders = zip(
        *(doubled(value_grad[:, c * width : (c + 1) * width], way) for c, way in enumerate(ways))
    )
    theirs = [lax.ppermute(piece, "seq", [(0, 1), (1, 0)]) for piece in mine]
    far, near = gathered(activations, turned)
    owned = [
        lax.all_to_all(part, ("dp", "seq"), 0, 0, tiled=True).reshape(members, 2, -1, rows_here)
        for part in (far, near)
    ]
    sent = owner_sum(owned[0], mine, theirs, orders, None, jnp.bfloat16)
    arrived = lax.ppermute(sent, "half", [(0, 1), (1, 0)])
    return owner_sum(owned[1], mine, theirs, orders, arrived, jnp.float32)


def solution(mesh):
    dp, seq = mesh.devices.shape
    split = jax.sharding.Mesh(mesh.devices.reshape(2, dp // 2, seq), ("half", "dp", "seq"))
    whole = ("half", "dp", "seq")
    return jax.shard_map(
        body,
        mesh=split,
        in_specs=(P(whole, None),) * 4 + (P(),),
        out_specs=P(whole, None),
        check_vma=False,
    )
```

```python
import functools

import jax
import jax.numpy as jnp
from jax import lax
from jax.experimental import pallas as pl
from jax.experimental.pallas import tpu as pltpu
from jax.sharding import PartitionSpec as P


H = 64
KVH = 8
HD = 128


def passed_along(value, axis, steps):
    count = lax.axis_size(axis)
    initial, last = (max(0, -steps), min(count, count - steps))
    return lax.ppermute(value, axis, [(source, source + steps) for source in range(initial, last)])


def gather_kernel(layout_ref, act_ref, out_ref, flipped, picked):
    width = act_ref.shape[1]
    step = 512

    def flip(i, carry):
        at = pl.multiple_of(i * step, step)
        flipped[pl.ds(at, step), :] = act_ref[:, pl.ds(at, step)].astype(jnp.float32).T
        return carry

    lax.fori_loop(0, width // step, flip, 0)
    rows = 256

    def pick(i, carry):
        at = pl.multiple_of(i * rows, rows)

        def some(j, inner):
            first = pl.multiple_of(j * 32, 32)
            for k in range(32):
                row = layout_ref[at + first + k]
                picked[pl.ds(first + k, 1), :] = flipped[pl.ds(row, 1), :]
            return inner

        lax.fori_loop(0, rows // 32, some, 0)
        out_ref[pl.ds(at, rows), :] = picked[...].astype(jnp.bfloat16)
        return carry

    lax.fori_loop(0, out_ref.shape[0] // rows, pick, 0)


def gathered(activations, layout):
    tokens, width = activations.shape
    return pl.pallas_call(
        gather_kernel,
        out_shape=jax.ShapeDtypeStruct((layout.shape[0], tokens), jnp.bfloat16),
        in_specs=[
            pl.BlockSpec(memory_space=pltpu.SMEM),
            pl.BlockSpec(memory_space=pltpu.VMEM),
        ],
        out_specs=pl.BlockSpec(memory_space=pltpu.VMEM),
        scratch_shapes=[
            pltpu.VMEM((width, tokens), jnp.float32),
            pltpu.VMEM((256, tokens), jnp.float32),
        ],
        cost_estimate=pl.CostEstimate(
            flops=8 * 10**9, bytes_accessed=20 * 2**20, transcendentals=0
        ),
    )(layout, activations)


def attention_kernel(q_ref, early_ref, keys_ref, grad_ref, out_ref, *, per_group):
    tokens = q_ref.shape[0]
    seq_index = lax.axis_index("seq")
    both_keys = jnp.concatenate([early_ref[...], keys_ref[...]], axis=0)
    place = lax.broadcasted_iota(jnp.int32, (tokens, 2 * tokens), 0)
    other = lax.broadcasted_iota(jnp.int32, (tokens, 2 * tokens), 1)
    allowed = (other <= place + tokens) & (other >= jnp.where(seq_index == 0, tokens, 0))
    total = jnp.zeros((2 * tokens, HD), jnp.float32)
    for head in range(per_group):
        columns = slice(head * HD, (head + 1) * HD)
        scores = lax.dot_general(
            q_ref[:, columns], both_keys, (((1,), (1,)), ((), ())),
            preferred_element_type=jnp.float32,
        ) * (1.0 / float(HD) ** 0.5)
        scores = jnp.where(allowed, scores, -jnp.inf)
        powers = jnp.exp(scores - jnp.max(scores, axis=1, keepdims=True))
        weights = (powers / jnp.sum(powers, axis=1, keepdims=True)).astype(jnp.bfloat16)
        total += lax.dot_general(
            weights, grad_ref[:, columns], (((0,), (0,)), ((), ())),
            preferred_element_type=jnp.float32,
        )
    out_ref[...] = total


def partial_values(queries, earlier, keys, out_grad):
    tokens = queries.shape[0]
    per_group = H // KVH
    wide = pl.BlockSpec((tokens, per_group * HD), lambda g: (0, g))
    narrow = pl.BlockSpec((tokens, HD), lambda g: (0, g))
    return pl.pallas_call(
        functools.partial(attention_kernel, per_group=per_group),
        grid=(KVH,),
        out_shape=jax.ShapeDtypeStruct((2 * tokens, KVH * HD), jnp.float32),
        in_specs=[wide, narrow, narrow, wide],
        out_specs=pl.BlockSpec((2 * tokens, HD), lambda g: (0, g)),
        cost_estimate=pl.CostEstimate(
            flops=8 * 10**9, bytes_accessed=20 * 2**20, transcendentals=2**21
        ),
    )(queries, earlier, keys, out_grad)


def sum_kernel(*refs, orders, add):
    owned_ref = refs[0]
    colors = len(orders)
    mine, theirs = refs[1 : 1 + colors], refs[1 + colors : 1 + 2 * colors]
    out_ref = refs[-1]
    me, seq_index = lax.axis_index("dp"), lax.axis_index("seq")
    for color, order in enumerate(orders):
        width = mine[color].shape[2]
        columns = slice(color * width, (color + 1) * width)
        if add:
            total = refs[-2][:, columns].astype(jnp.float32)
        else:
            total = jnp.zeros((owned_ref.shape[2], width), jnp.float32)
        for place, step in enumerate(order):
            source = me ^ step
            left = jnp.concatenate(
                [owned_ref[source, seq_index], owned_ref[source, 1 - seq_index]], axis=1
            )
            right = jnp.concatenate([mine[color][place], theirs[color][place]], axis=0)
            total += jnp.dot(left, right, preferred_element_type=jnp.float32)
        out_ref[:, columns] = total.astype(out_ref.dtype)


def owner_sum(owned, mine, theirs, orders, arrived, kind):
    rows = owned.shape[2]
    width = sum(piece.shape[2] for piece in mine)
    extra = [] if arrived is None else [arrived]
    operands = [owned, *mine, *theirs, *extra]
    return pl.pallas_call(
        functools.partial(sum_kernel, orders=orders, add=arrived is not None),
        out_shape=jax.ShapeDtypeStruct((rows, width), kind),
        in_specs=[pl.BlockSpec(memory_space=pltpu.VMEM)] * len(operands),
        out_specs=pl.BlockSpec(memory_space=pltpu.VMEM),
        cost_estimate=pl.CostEstimate(
            flops=2 * owned.size * width, bytes_accessed=6 * 2**20, transcendentals=0
        ),
        compiler_params=pltpu.CompilerParams(vmem_limit_bytes=56 * 2**20),
    )(*operands)


def doubled(piece, bits):
    count = lax.axis_size("dp")
    held, order = piece[None], [0]
    for bit in bits:
        arrived = lax.ppermute(held, "dp", [(i, i ^ bit) for i in range(count)])
        held = jnp.concatenate([held, arrived], axis=0)
        order = order + [step ^ bit for step in order]
    return held, tuple(order)


def body(activations, queries, keys, out_grad, layout):
    rows_here = activations.shape[0]
    members, halves = lax.axis_size("dp"), lax.axis_size("half")
    half = lax.axis_index("half")
    split = layout.shape[0] // halves
    turned = jnp.where(half == 0, jnp.roll(layout, -split), layout)
    earlier = passed_along(keys, "seq", 1)
    far = gathered(activations, turned[:split])
    far_owned = lax.all_to_all(far, ("dp", "seq"), 0, 0, tiled=True)
    far, queries = lax.optimization_barrier((far, queries))
    partial = partial_values(queries, earlier, keys, out_grad)
    returned = passed_along(partial[:rows_here], "seq", -1)
    value_grad = (partial[rows_here:] + returned).astype(jnp.bfloat16)
    value_grad, activations = lax.optimization_barrier((value_grad, activations))
    near = gathered(activations, turned[split:])
    bits = [1 << k for k in reversed(range(members.bit_length() - 1))]
    ways = [bits, bits[:-2] + bits[-2:][::-1]]
    width = value_grad.shape[1] // len(ways)
    mine, orders = zip(
        *(doubled(value_grad[:, c * width : (c + 1) * width], way) for c, way in enumerate(ways))
    )
    near, *mine = lax.optimization_barrier((near, *mine))
    theirs = [lax.ppermute(piece, "seq", [(0, 1), (1, 0)]) for piece in mine]
    near_owned = lax.all_to_all(near, ("dp", "seq"), 0, 0, tiled=True)
    owned = [part.reshape(members, 2, -1, rows_here) for part in (far_owned, near_owned)]
    sent = owner_sum(owned[0], mine, theirs, orders, None, jnp.bfloat16)
    arrived = lax.ppermute(sent, "half", [(0, 1), (1, 0)])
    return owner_sum(owned[1], mine, theirs, orders, arrived, jnp.float32)


def solution(mesh):
    dp, seq = mesh.devices.shape
    split = jax.sharding.Mesh(mesh.devices.reshape(2, dp // 2, seq), ("half", "dp", "seq"))
    whole = ("half", "dp", "seq")
    return jax.shard_map(
        body,
        mesh=split,
        in_specs=(P(whole, None),) * 4 + (P(),),
        out_specs=P(whole, None),
        check_vma=False,
    )
```
